256 devices in a mesh: tm: 32 (over z, x_hi, core), rows: 8 (over x_lo, y).
Axes of the slice: x: 4 (x_hi: 2, x_lo: 2; x = x_hi * 2 + x_lo), y: 4, z: 8, core: 2. Of those that a mesh axis runs over, the one named last changes fastest.
Arguments:
- frames: bfloat16 [64, 64, 128, 128], P('tm', 'rows'), may hold values from -6 to 6
- conv_fine: bfloat16 [3, 3, 384, 128], replicated, may hold values from -0.109375 to 0.109375
- conv_down: bfloat16 [3, 384, 256], replicated, may hold values from -0.1875 to 0.1875
- conv_coarse: bfloat16 [3, 3, 768, 256], replicated, may hold values from -0.078125 to 0.078125
Outputs:
- coarse_out: bfloat16 [32, 32, 64, 256], P('tm', 'rows')
The draws below stay inside these ranges and needn't reach their ends.
All inputs are finite; a program needn't handle non-finite values.
Results may differ from the reference program's by a relative error of at most 0.014.
Values may be sent and summed in bfloat16 or wider, within the bound.
A program may use at most 64 MiB of HBM per device.

```python
import jax
import jax.numpy as jnp
from jax import lax

C1 = 128
C2 = 256
COLS = 128
FRAMES = 64
ROWS = 64


def shard_levels(key, shape, split, least, top_value):
    def one(position, parts):
        draws = jax.random.uniform(jax.random.fold_in(jax.random.fold_in(key, 6), position), (parts,), jnp.float32, least / len(split), top_value / len(split))
        return jnp.repeat(jnp.exp(draws), shape[position] // parts).reshape((-1,) + (1,) * (len(shape) - position - 1))

    level = one(*split[0])
    for cut in split[1:]:
        level = level * one(*cut)
    return level


def noise(key, shape, spread, bound, cuts=(), dtype=jnp.bfloat16):
    drawn = spread * jax.random.normal(key, shape, jnp.float32)
    if cuts:
        drawn = drawn * shard_levels(key, shape, cuts, -0.22, 0.18)
    return jnp.clip(drawn, -bound, bound).astype(dtype)


def setup_inputs(seed: int = 0) -> dict:
    seeds = jax.random.split(jax.random.key(seed), 5)
    return {
        "frames": noise(seeds[0], (FRAMES, ROWS, COLS, C1), 1.0, 6.0, ((0, 32), (1, 8))),
        "conv_fine": noise(seeds[1], (3, 3, 3 * C1, C1), (27 * C1) ** -0.5, 0.109375),
        "conv_down": noise(seeds[2], (3, 3 * C1, C2), (9 * C1) ** -0.5, 0.1875),
        "conv_coarse": noise(seeds[3], (3, 3, 3 * C2, C2), (27 * C2) ** -0.5, 0.078125),
    }


def conv_causal(field, weight, channels):
    kernel = weight.reshape(3, 3, 3, channels, weight.shape[-1])
    padded = jnp.pad(field, ((2, 0), (1, 1), (1, 1), (0, 0)))
    result = lax.conv_general_dilated(padded[None], kernel, (1, 1, 1), "VALID", dimension_numbers=("NDHWC", "DHWIO", "NDHWC"), preferred_element_type=jnp.float32)
    return result[0]


def reference(frames, conv_fine, conv_down, conv_coarse):
    fine_out = jax.nn.silu(conv_causal(frames, conv_fine, C1)).astype(jnp.bfloat16)
    frame_pairs = fine_out.astype(jnp.float32).reshape(FRAMES // 2, 2, ROWS, COLS, C1)
    pooled = ((frame_pairs[:, 0] + frame_pairs[:, 1]) * 0.5).astype(jnp.bfloat16)
    padded = jnp.pad(pooled, ((0, 0), (0, 1), (0, 1), (0, 0)))
    kernel = conv_down.reshape(3, 3, C1, C2)
    reduced = lax.conv_general_dilated(padded, kernel, (2, 2), "VALID", dimension_numbers=("NHWC", "HWIO", "NHWC"), preferred_element_type=jnp.float32).astype(jnp.bfloat16)
    coarse_out = jax.nn.silu(conv_causal(reduced, conv_coarse, C2)).astype(jnp.bfloat16)
    return coarse_out
```

```python
import jax
import jax.numpy as jnp
from jax import lax
from jax.experimental import pallas as pl
from jax.experimental.pallas import tpu as pltpu
from jax.sharding import PartitionSpec as P

MESH = pl.DeviceIdType.MESH
F32 = jnp.float32
BF16 = jnp.bfloat16

E0, E1, M0, M1, OU, OD, FU, FD, PR = range(9)
N1A, N1B, N2A, N2B, T2U, T2D, T1U, T1D, T0U, T0D = range(9, 19)
HA, HB, S0, S1 = 19, 20, 21, 22
COPIES = 23


def silu(v):
    return v / (1.0 + jnp.exp(-v))


def spread(y0, y1, y2, cols):
    col = lax.broadcasted_iota(jnp.int32, y0.shape, 0) % cols
    left = jnp.where(col == 0, 0.0, pltpu.roll(y0, 1, 0))
    right = jnp.where(col == cols - 1, 0.0, pltpu.roll(y2, y2.shape[0] - 1, 0))
    return left + y1 + right


def dot(a, b):
    return jnp.dot(a, b, preferred_element_type=F32)


def kernel(
    tms, rws, frames, wf_h, wd_h, wc_h, out, x, wf, wd, wc, z, pool, red, y, ssem, rsem, lsem
):
    tm = lax.axis_index("tm")
    row = lax.axis_index("rows")
    core = tm % 2
    has_next, has_prev = tm < tms - 1, tm > 0
    has_prev2 = tm > 1
    up, down = row > 0, row < rws - 1
    first = core == 0
    hop2 = first & (tm < tms - 2)
    from2 = first & has_prev2

    barrier = pltpu.get_barrier_semaphore()
    total = jnp.int32(0)
    for ok, dev in (
        (has_next, (tm + 1, row)),
        (has_prev, (tm - 1, row)),
        (up, (tm, row - 1)),
        (down, (tm, row + 1)),
        (hop2, (tm + 2, row)),
        (from2, (tm - 2, row)),
    ):

        @pl.when(ok)
        def _():
            pl.semaphore_signal(barrier, inc=1, device_id=dev, device_id_type=MESH)

        total = total + ok.astype(jnp.int32)

    loads = [
        pltpu.make_async_copy(frames, x.at[pl.ds(2, 2), pl.ds(1, 8)], lsem.at[0]),
        pltpu.make_async_copy(wf_h, wf, lsem.at[1]),
        pltpu.make_async_copy(wd_h, wd, lsem.at[2]),
        pltpu.make_async_copy(wc_h, wc, lsem.at[3]),
    ]
    for load in loads:
        load.start()

    pool[:, pl.ds(128, 8), :] = jnp.zeros((9, 8, 128), F32)

    @pl.when(~up)
    def _():
        x[:, 0] = jnp.zeros((4, 128, 128), BF16)
        red[:, 0] = jnp.zeros((3, 64, 256), BF16)

    @pl.when(~down)
    def _():
        x[:, 9] = jnp.zeros((4, 128, 128), BF16)
        red[:, 5] = jnp.zeros((3, 64, 256), BF16)
        pool[8, pl.ds(0, 128)] = jnp.zeros((128, 128), F32)

    @pl.when(~has_prev)
    def _():
        x[0:2, pl.ds(1, 8)] = jnp.zeros((2, 8, 128, 128), BF16)
        red[1, pl.ds(1, 4)] = jnp.zeros((4, 64, 256), BF16)

        @pl.when(up)
        def _():
            x[0:2, 0] = jnp.zeros((2, 128, 128), BF16)
            red[1, 0] = jnp.zeros((64, 256), BF16)

        @pl.when(down)
        def _():
            x[0:2, 9] = jnp.zeros((2, 128, 128), BF16)
            red[1, 5] = jnp.zeros((64, 256), BF16)

    @pl.when(~has_prev2)
    def _():
        red[0, pl.ds(1, 4)] = jnp.zeros((4, 64, 256), BF16)

        @pl.when(up)
        def _():
            red[0, 0] = jnp.zeros((64, 256), BF16)

        @pl.when(down)
        def _():
            red[0, 5] = jnp.zeros((64, 256), BF16)

    def remote(k, src, dst, dev, recv=None):
        return pltpu.make_async_remote_copy(
            src_ref=src,
            dst_ref=dst,
            send_sem=ssem.at[k],
            recv_sem=rsem.at[k if recv is None else recv],
            device_id=dev,
            device_id_type=MESH,
        )

    sent = []

    def send(ok, copy):
        @pl.when(ok)
        def _():
            copy.start()

        sent.append((ok, copy))

    def arrived(ok, copy):
        @pl.when(ok)
        def _():
            copy.wait_recv()

    nxt, nx2 = (tm + 1, row), (tm + 2, row)
    above, below = (tm, row - 1), (tm, row + 1)
    own, old = pl.ds(2, 2), pl.ds(0, 2)
    c = {
        E0: remote(E0, x.at[own, pl.ds(1, 1)], x.at[old, pl.ds(1, 1)], nxt),
        E1: remote(E1, x.at[own, pl.ds(8, 1)], x.at[old, pl.ds(8, 1)], nxt),
        S0: remote(S0, x.at[own, pl.ds(2, 1)], x.at[old, pl.ds(2, 1)], nxt),
        S1: remote(S1, x.at[own, pl.ds(7, 1)], x.at[old, pl.ds(7, 1)], nxt),
        M0: remote(M0, x.at[own, pl.ds(3, 2)], x.at[old, pl.ds(3, 2)], nxt),
        M1: remote(M1, x.at[own, pl.ds(5, 2)], x.at[old, pl.ds(5, 2)], nxt),
        OU: remote(OU, x.at[own, pl.ds(1, 1)], x.at[own, pl.ds(9, 1)], above),
        OD: remote(OD, x.at[own, pl.ds(8, 1)], x.at[own, pl.ds(0, 1)], below),
        FU: remote(FU, x.at[old, pl.ds(1, 1)], x.at[old, pl.ds(9, 1)], above),
        FD: remote(FD, x.at[old, pl.ds(8, 1)], x.at[old, pl.ds(0, 1)], below),
        PR: remote(PR, pool.at[0, pl.ds(0, 128)], pool.at[8, pl.ds(0, 128)], above),
        N1A: remote(N1A, red.at[2, pl.ds(1, 3)], red.at[1, pl.ds(1, 3)], nxt),
        N1B: remote(N1B, red.at[2, pl.ds(4, 1)], red.at[1, pl.ds(4, 1)], nxt),
        T2U: remote(T2U, red.at[2, pl.ds(1, 1)], red.at[2, pl.ds(5, 1)], above),
        T2D: remote(T2D, red.at[2, pl.ds(4, 1)], red.at[2, pl.ds(0, 1)], below),
        T1U: remote(T1U, red.at[1, pl.ds(1, 1)], red.at[1, pl.ds(5, 1)], above),
        T1D: remote(T1D, red.at[1, pl.ds(4, 1)], red.at[1, pl.ds(0, 1)], below),
        T0U: remote(T0U, red.at[0, pl.ds(1, 1)], red.at[0, pl.ds(5, 1)], above),
        T0D: remote(T0D, red.at[0, pl.ds(4, 1)], red.at[0, pl.ds(0, 1)], below),
    }
    far_a = remote(N2A, red.at[2, pl.ds(1, 3)], red.at[0, pl.ds(1, 3)], nx2)
    far_b = remote(N2B, red.at[2, pl.ds(4, 1)], red.at[0, pl.ds(4, 1)], nx2)
    hand_a = remote(HA, red.at[1, pl.ds(1, 3)], red.at[0, pl.ds(1, 3)], nxt, N2A)
    hand_b = remote(HB, red.at[1, pl.ds(4, 1)], red.at[0, pl.ds(4, 1)], nxt, N2B)

    def tap(a, b, e):
        return wf[a, b, pl.ds(e * 128, 128), :]

    def fine(lhs, main, side, both, single, other):
        left = jnp.concatenate(
            [lhs(main, b) for b in range(3)] + [lhs(side, b) for b in range(3)], axis=1
        )

        def rhs(pairs):
            return jnp.concatenate([jnp.concatenate(pair, axis=1) for pair in pairs], axis=0)

        none = jnp.zeros((128, 128), BF16)
        n0 = dot(
            left,
            rhs(
                [(tap(both, b, 0), tap(both, b, 1)) for b in range(3)]
                + [(tap(single, b, 0), tap(single, b, 1)) for b in range(3)]
            ),
        )
        n1 = dot(
            left,
            rhs(
                [(tap(both, b, 2), tap(other, b, 0)) for b in range(3)]
                + [(tap(single, b, 2), none) for b in range(3)]
            ),
        )
        n2 = dot(left[:, :384], rhs([(tap(other, b, 1), tap(other, b, 2)) for b in range(3)]))
        mine = spread(n0[:, :128], n0[:, 128:], n1[:, :128], 128)
        rest = spread(n1[:, 128:], n2[:, :128], n2[:, 128:], 128)
        return mine, rest

    def late(lhs):
        second, head = fine(lhs, 2, 3, 1, 2, 2)
        return head, second

    def early(lhs):
        return fine(lhs, 1, 0, 1, 0, 0)

    def pooled(head, second):
        a = silu(head).astype(BF16).astype(F32)
        b = silu(second).astype(BF16).astype(F32)
        return ((a + b) * 0.5).astype(BF16).astype(F32)

    def inner(r):
        return lambda f, b: x[f, pl.ds(r + b, 2)].reshape(256, 128)

    def edges(f, b):
        return jnp.concatenate([x[f, b], x[f, 7 + b]], axis=0)

    loads[0].wait()
    loads[1].wait()

    def own_part(i, carry):
        r = 2 * i + 1
        head, second = late(inner(r))
        z[0, pl.ds(r, 2)] = head.reshape(2, 128, 128)
        z[1, pl.ds(r, 2)] = second.reshape(2, 128, 128)
        return carry

    lax.fori_loop(0, 3, own_part, 0)
    pl.semaphore_wait(barrier, total)

    send(up, c[OU])
    send(down, c[OD])
    for k in (E0, E1, S0, S1, M0, M1):
        send(has_next, c[k])

    arrived(has_prev, c[E0])
    send(up & has_prev, c[FU])
    arrived(has_prev, c[E1])
    send(down & has_prev, c[FD])
    arrived(down, c[OU])
    arrived(up, c[OD])
    arrived(down & has_prev, c[FU])
    arrived(up & has_prev, c[FD])
    arrived(has_prev, c[S0])
    arrived(has_prev, c[S1])

    head_a, second_a = late(edges)
    head_b, second_b = early(edges)
    ends = pooled(head_a + head_b, second_a + second_b)
    pool[0, pl.ds(0, 128)] = ends[:128]
    pool[7, pl.ds(0, 128)] = ends[128:]
    send(up, c[PR])

    def rest_part(i, carry):
        r = 2 * i + 1
        head, second = early(inner(r))
        head = head + z[0, pl.ds(r, 2)].reshape(256, 128)
        second = second + z[1, pl.ds(r, 2)].reshape(256, 128)
        pool[pl.ds(r, 2), pl.ds(0, 128)] = pooled(head, second).reshape(2, 128, 128)
        return carry

    arrived(has_prev, c[M0])
    rest_part(0, 0)
    arrived(has_prev, c[M1])
    lax.fori_loop(1, 3, rest_part, 0)

    loads[2].wait()
    arrived(down, c[PR])
    weight = wd[...].reshape(1152, 256)
    strips = [
        jnp.concatenate(
            [
                pool[2 * p + b, pl.ds(e, 64, stride=2), :].astype(BF16)
                for b in range(3)
                for e in range(3)
            ],
            axis=1,
        )
        for p in range(4)
    ]
    red[2, pl.ds(1, 4)] = (
        dot(jnp.concatenate(strips, axis=0), weight).astype(BF16).reshape(4, 64, 256)
    )

    send(up, c[T2U])
    send(down, c[T2D])
    send(has_next, c[N1A])
    send(hop2, far_a)
    send(has_next, c[N1B])
    send(hop2, far_b)

    loads[3].wait()
    arrived(down, c[T2U])
    arrived(up, c[T2D])

    def coarse(a, e):
        left = jnp.concatenate(
            [red[a, pl.ds(b, 4)].reshape(256, 256) for b in range(3)], axis=1
        )
        right = jnp.concatenate([wc[a, b, pl.ds(e * 256, 256), :] for b in range(3)], axis=0)
        return dot(left, right)

    for e in range(3):
        y[e] = coarse(2, e)

    hand = first & has_prev
    arrived(has_prev, c[N1A])
    send(hand, hand_a)
    send(up & has_prev, c[T1U])
    arrived(has_prev, c[N1B])
    send(hand, hand_b)
    send(down & has_prev, c[T1D])
    arrived(has_prev2, far_a)
    send(up & has_prev2, c[T0U])
    arrived(has_prev2, far_b)
    send(down & has_prev2, c[T0D])
    arrived(down & has_prev, c[T1U])
    arrived(up & has_prev, c[T1D])
    for e in range(3):
        y[e] = y[e] + coarse(1, e)
    arrived(down & has_prev2, c[T0U])
    arrived(up & has_prev2, c[T0D])
    parts = [y[e] + coarse(0, e) for e in range(3)]
    out[...] = silu(spread(*parts, 64)).astype(BF16).reshape(1, 4, 64, 256)

    for ok, copy in sent:

        @pl.when(ok)
        def _():
            copy.wait_send()


def solution(mesh):
    import functools

    tms, rws = mesh.shape["tm"], mesh.shape["rows"]
    anywhere = pl.BlockSpec(memory_space=pl.ANY)

    def local(frames, conv_fine, conv_down, conv_coarse):
        return pl.pallas_call(
            functools.partial(kernel, tms, rws),
            out_shape=jax.ShapeDtypeStruct((1, 4, 64, 256), BF16),
            in_specs=[anywhere] * 4,
            out_specs=pl.BlockSpec(memory_space=pltpu.VMEM),
            scratch_shapes=[
                pltpu.VMEM((4, 10, 128, 128), BF16),
                pltpu.VMEM((3, 3, 384, 128), BF16),
                pltpu.VMEM((3, 384, 256), BF16),
                pltpu.VMEM((3, 3, 768, 256), BF16),
                pltpu.VMEM((2, 8, 128, 128), F32),
                pltpu.VMEM((9, 136, 128), F32),
                pltpu.VMEM((3, 6, 64, 256), BF16),
                pltpu.VMEM((3, 256, 256), F32),
                pltpu.SemaphoreType.DMA((COPIES,)),
                pltpu.SemaphoreType.DMA((COPIES,)),
                pltpu.SemaphoreType.DMA((4,)),
            ],
            compiler_params=pltpu.CompilerParams(
                collective_id=0, has_side_effects=True, vmem_limit_bytes=60 * 1024 * 1024
            ),
            name="encoder",
        )(frames, conv_fine, conv_down, conv_coarse)

    placed = (P("tm", "rows", None, None), P(), P(), P())
    return jax.shard_map(
        local, mesh=mesh, in_specs=placed, out_specs=P("tm", "rows", None, None), check_vma=False
    )
```

```python
import jax
import jax.numpy as jnp
from jax import lax
from jax.experimental import pallas as pl
from jax.experimental.pallas import tpu as pltpu
from jax.sharding import PartitionSpec as P

MESH = pl.DeviceIdType.MESH
F32 = jnp.float32
BF16 = jnp.bfloat16

NAMES = (
    "E0", "E1", "S0", "M0", "M1", "OU", "OD", "FU", "FD", "HU", "HD", "PR",
    "NU", "ND", "NM", "QU", "QD", "QM", "GU", "GD", "GM", "T2U", "T2D", "T1U",
    "T1D", "T0U", "T0D", "K1U", "K1D", "K0U", "K0D",
)
IDS = {name: i for i, name in enumerate(NAMES)}


def silu(v):
    return v / (1.0 + jnp.exp(-v))


def spread(y0, y1, y2, cols):
    col = lax.broadcasted_iota(jnp.int32, y0.shape, 0) % cols
    left = jnp.where(col == 0, 0.0, pltpu.roll(y0, 1, 0))
    right = jnp.where(col == cols - 1, 0.0, pltpu.roll(y2, y2.shape[0] - 1, 0))
    return left + y1 + right


def dot(a, b):
    return jnp.dot(a, b, preferred_element_type=F32)


def kernel(
    tms, rws, frames, wf_h, wd_h, wc_h, out, x, wf, wd, wc, z, pool, rim, red, y, ssem, rsem, lsem
):
    tm = lax.axis_index("tm")
    row = lax.axis_index("rows")
    first = tm % 2 == 0
    second = ~first
    has_next, has_prev = tm < tms - 1, tm > 0
    has_next2, has_prev2 = tm < tms - 2, tm > 1
    up, down = row > 0, row < rws - 1
    half = rws // 2
    cross_up, cross_down = row == half, row == half - 1

    barrier = pltpu.get_barrier_semaphore()
    total = jnp.int32(0)
    for ok, dev in (
        (has_next, (tm + 1, row)),
        (has_prev, (tm - 1, row)),
        (up, (tm, row - 1)),
        (down, (tm, row + 1)),
        (first & has_next2, (tm + 2, row)),
        (first & has_prev2, (tm - 2, row)),
        (second & has_next & cross_up, (tm + 1, row - 1)),
        (second & has_next & cross_down, (tm + 1, row + 1)),
        (first & has_prev & cross_up, (tm - 1, row - 1)),
        (first & has_prev & cross_down, (tm - 1, row + 1)),
        (first & has_next2 & cross_up, (tm + 2, row - 1)),
        (first & has_next2 & cross_down, (tm + 2, row + 1)),
        (first & has_prev2 & cross_up, (tm - 2, row - 1)),
        (first & has_prev2 & cross_down, (tm - 2, row + 1)),
    ):

        @pl.when(ok)
        def _():
            pl.semaphore_signal(barrier, inc=1, device_id=dev, device_id_type=MESH)

        total = total + ok.astype(jnp.int32)

    loads = [
        pltpu.make_async_copy(frames, x.at[pl.ds(2, 2), pl.ds(1, 8)], lsem.at[0]),
        pltpu.make_async_copy(wf_h, wf, lsem.at[1]),
        pltpu.make_async_copy(wd_h, wd, lsem.at[2]),
        pltpu.make_async_copy(wc_h, wc, lsem.at[3]),
    ]
    for load in loads:
        load.start()

    pool[:, pl.ds(128, 8), :] = jnp.zeros((9, 8, 128), F32)

    @pl.when(~up)
    def _():
        x[:, 0] = jnp.zeros((4, 128, 128), BF16)
        red[:, 0] = jnp.zeros((3, 64, 256), BF16)

    @pl.when(~down)
    def _():
        x[:, 9] = jnp.zeros((4, 128, 128), BF16)
        red[:, 5] = jnp.zeros((3, 64, 256), BF16)
        rim[1] = jnp.zeros((128, 128), BF16)

    @pl.when(~has_prev)
    def _():
        x[0:2, pl.ds(1, 8)] = jnp.zeros((2, 8, 128, 128), BF16)
        red[1, pl.ds(1, 4)] = jnp.zeros((4, 64, 256), BF16)

        @pl.when(up)
        def _():
            x[0:2, 0] = jnp.zeros((2, 128, 128), BF16)
            red[1, 0] = jnp.zeros((64, 256), BF16)

        @pl.when(down)
        def _():
            x[0:2, 9] = jnp.zeros((2, 128, 128), BF16)
            red[1, 5] = jnp.zeros((64, 256), BF16)

    @pl.when(~has_prev2)
    def _():
        red[0, pl.ds(1, 4)] = jnp.zeros((4, 64, 256), BF16)

        @pl.when(up)
        def _():
            red[0, 0] = jnp.zeros((64, 256), BF16)

        @pl.when(down)
        def _():
            red[0, 5] = jnp.zeros((64, 256), BF16)

    sent = []

    def send(ok, name, src, dst, dev, recv=None):
        copy = pltpu.make_async_remote_copy(
            src_ref=src,
            dst_ref=dst,
            send_sem=ssem.at[IDS[name]],
            recv_sem=rsem.at[IDS[recv or name]],
            device_id=dev,
            device_id_type=MESH,
        )

        @pl.when(ok)
        def _():
            copy.start()

        sent.append((ok, copy))

    def arrived(ok, name, dst):
        copy = pltpu.make_async_remote_copy(
            src_ref=dst,
            dst_ref=dst,
            send_sem=ssem.at[IDS[name]],
            recv_sem=rsem.at[IDS[name]],
            device_id=nxt,
            device_id_type=MESH,
        )

        @pl.when(ok)
        def _():
            copy.wait_recv()

    nxt, nx2 = (tm + 1, row), (tm + 2, row)
    above, below = (tm, row - 1), (tm, row + 1)

    def own(r, n=1):
        return x.at[pl.ds(2, 2), pl.ds(r, n)]

    def old(r, n=1):
        return x.at[pl.ds(0, 2), pl.ds(r, n)]

    def part(a, r, n=1):
        return red.at[a, pl.ds(r, n)]

    def tap(a, b, e):
        return wf[a, b, pl.ds(e * 128, 128), :]

    def fine(lhs, main, side, both, single, other):
        left = jnp.concatenate(
            [lhs(main, b) for b in range(3)] + [lhs(side, b) for b in range(3)], axis=1
        )

        def rhs(pairs):
            return jnp.concatenate([jnp.concatenate(pair, axis=1) for pair in pairs], axis=0)

        none = jnp.zeros((128, 128), BF16)
        n0 = dot(
            left,
            rhs(
                [(tap(both, b, 0), tap(both, b, 1)) for b in range(3)]
                + [(tap(single, b, 0), tap(single, b, 1)) for b in range(3)]
            ),
        )
        n1 = dot(
            left,
            rhs(
                [(tap(both, b, 2), tap(other, b, 0)) for b in range(3)]
                + [(tap(single, b, 2), none) for b in range(3)]
            ),
        )
        n2 = dot(left[:, :384], rhs([(tap(other, b, 1), tap(other, b, 2)) for b in range(3)]))
        mine = spread(n0[:, :128], n0[:, 128:], n1[:, :128], 128)
        rest = spread(n1[:, 128:], n2[:, :128], n2[:, 128:], 128)
        return mine, rest

    def late(lhs):
        second, head = fine(lhs, 2, 3, 1, 2, 2)
        return head, second

    def early(lhs):
        return fine(lhs, 1, 0, 1, 0, 0)

    def pooled(head, second):
        a = silu(head).astype(BF16).astype(F32)
        b = silu(second).astype(BF16).astype(F32)
        return ((a + b) * 0.5).astype(BF16).astype(F32)

    def inner(r):
        return lambda f, b: x[f, pl.ds(r + b, 2)].reshape(256, 128)

    loads[0].wait()
    loads[1].wait()

    def own_part(i, carry):
        r = 2 * i + 1
        head, second = late(inner(r))
        z[0, pl.ds(r, 2)] = head.reshape(2, 128, 128)
        z[1, pl.ds(r, 2)] = second.reshape(2, 128, 128)
        return carry

    lax.fori_loop(0, 3, own_part, 0)
    pl.semaphore_wait(barrier, total)

    far = first & has_prev
    lead = second & has_next
    send(up, "OU", own(1), own(9), above)
    send(down, "OD", own(8), own(0), below)
    send(lead & cross_up, "FU", own(1), old(9), (tm + 1, row - 1))
    send(lead & cross_down, "FD", own(8), old(0), (tm + 1, row + 1))
    send(has_next, "E0", own(1), old(1), nxt)
    send(has_next, "E1", own(8), old(8), nxt)
    send(has_next, "S0", own(2), old(2), nxt)
    send(has_next, "M0", own(3, 2), old(3, 2), nxt)
    send(has_next, "M1", own(5, 3), old(5, 3), nxt)

    arrived(down, "OU", own(9))
    send(first & down, "HU", own(9), old(9), nxt, "FU")
    arrived(up, "OD", own(0))
    send(first & up, "HD", own(0), old(0), nxt, "FD")
    arrived(has_prev, "E0", old(1))
    send(far & up & ~cross_up, "FU", old(1), old(9), above)
    arrived(has_prev, "E1", old(8))
    send(far & down & ~cross_down, "FD", old(8), old(0), below)

    head_a, second_a = late(lambda f, b: jnp.concatenate([x[f, b], x[f, 7 + b]], axis=0))
    z[0, 7] = head_a[128:]
    z[1, 7] = second_a[128:]
    arrived(up & has_prev, "FD", old(0))
    arrived(has_prev, "S0", old(2))
    head_b, second_b = early(lambda f, b: x[f, b])
    top = pooled(head_a[:128] + head_b, second_a[:128] + second_b)
    pool[0, pl.ds(0, 128)] = top
    rim[0] = top.astype(BF16)
    send(up, "PR", rim.at[0], rim.at[1], above)

    def rest_part(i, carry):
        r = 2 * i + 1
        head, second = early(inner(r))
        head = head + z[0, pl.ds(r, 2)].reshape(256, 128)
        second = second + z[1, pl.ds(r, 2)].reshape(256, 128)
        pool[pl.ds(r, 2), pl.ds(0, 128)] = pooled(head, second).reshape(2, 128, 128)
        return carry

    arrived(has_prev, "M0", old(3, 2))
    rest_part(0, 0)
    arrived(has_prev, "M1", old(5, 3))
    lax.fori_loop(1, 3, rest_part, 0)
    arrived(down & has_prev, "FU", old(9))
    head_b, second_b = early(lambda f, b: x[f, 7 + b])
    pool[7, pl.ds(0, 128)] = pooled(z[0, 7] + head_b, z[1, 7] + second_b)

    loads[2].wait()
    arrived(down, "PR", rim.at[1])
    pool[8, pl.ds(0, 128)] = rim[1].astype(F32)
    weight = wd[...].reshape(1152, 256)
    strips = [
        jnp.concatenate(
            [
                pool[2 * p + b, pl.ds(e, 64, stride=2), :].astype(BF16)
                for b in range(3)
                for e in range(3)
            ],
            axis=1,
        )
        for p in range(4)
    ]
    red[2, pl.ds(1, 4)] = (
        dot(jnp.concatenate(strips, axis=0), weight).astype(BF16).reshape(4, 64, 256)
    )

    send(up, "T2U", part(2, 1), part(2, 5), above)
    send(down, "T2D", part(2, 4), part(2, 0), below)
    send(lead & cross_up, "T1U", part(2, 1), part(1, 5), (tm + 1, row - 1))
    send(lead & cross_down, "T1D", part(2, 4), part(1, 0), (tm + 1, row + 1))
    hop2 = first & has_next2
    send(hop2 & cross_up, "T0U", part(2, 1), part(0, 5), (tm + 2, row - 1))
    send(hop2 & cross_down, "T0D", part(2, 4), part(0, 0), (tm + 2, row + 1))
    send(has_next, "NU", part(2, 1), part(1, 1), nxt)
    send(has_next, "ND", part(2, 4), part(1, 4), nxt)
    send(hop2, "QU", part(2, 1), part(0, 1), nx2)
    send(hop2, "QD", part(2, 4), part(0, 4), nx2)
    send(has_next, "NM", part(2, 2, 2), part(1, 2, 2), nxt)
    send(hop2, "QM", part(2, 2, 2), part(0, 2, 2), nx2)

    def coarse(a, e):
        left = jnp.concatenate(
            [red[a, pl.ds(b, 4)].reshape(256, 256) for b in range(3)], axis=1
        )
        right = jnp.concatenate([wc[a, b, pl.ds(e * 256, 256), :] for b in range(3)], axis=0)
        return dot(left, right)

    loads[3].wait()
    arrived(down, "T2U", part(2, 5))
    send(first & down, "K1U", part(2, 5), part(1, 5), nxt, "T1U")
    arrived(up, "T2D", part(2, 0))
    send(first & up, "K1D", part(2, 0), part(1, 0), nxt, "T1D")
    for e in range(3):
        y[e] = coarse(2, e)

    far2 = first & has_prev2
    arrived(has_prev, "NU", part(1, 1))
    send(far & up & ~cross_up, "T1U", part(1, 1), part(1, 5), above)
    send(far, "GU", part(1, 1), part(0, 1), nxt, "QU")
    arrived(has_prev, "ND", part(1, 4))
    send(far & down & ~cross_down, "T1D", part(1, 4), part(1, 0), below)
    send(far, "GD", part(1, 4), part(0, 4), nxt, "QD")
    arrived(has_prev2, "QU", part(0, 1))
    send(far2 & up & ~cross_up, "T0U", part(0, 1), part(0, 5), above)
    arrived(has_prev2, "QD", part(0, 4))
    send(far2 & down & ~cross_down, "T0D", part(0, 4), part(0, 0), below)
    arrived(has_prev, "NM", part(1, 2, 2))
    send(far, "GM", part(1, 2, 2), part(0, 2, 2), nxt, "QM")
    arrived(down & has_prev, "T1U", part(1, 5))
    send(far & down, "K0U", part(1, 5), part(0, 5), nxt, "T0U")
    arrived(up & has_prev, "T1D", part(1, 0))
    send(far & up, "K0D", part(1, 0), part(0, 0), nxt, "T0D")
    for e in range(3):
        y[e] = y[e] + coarse(1, e)
    arrived(has_prev2, "QM", part(0, 2, 2))
    arrived(down & has_prev2, "T0U", part(0, 5))
    arrived(up & has_prev2, "T0D", part(0, 0))
    parts = [y[e] + coarse(0, e) for e in range(3)]
    out[...] = silu(spread(*parts, 64)).astype(BF16).reshape(1, 4, 64, 256)

    for ok, copy in sent:

        @pl.when(ok)
        def _():
            copy.wait_send()


def solution(mesh):
    import functools

    tms, rws = mesh.shape["tm"], mesh.shape["rows"]
    anywhere = pl.BlockSpec(memory_space=pl.ANY)

    def local(frames, conv_fine, conv_down, conv_coarse):
        return pl.pallas_call(
            functools.partial(kernel, tms, rws),
            out_shape=jax.ShapeDtypeStruct((1, 4, 64, 256), BF16),
            in_specs=[anywhere] * 4,
            out_specs=pl.BlockSpec(memory_space=pltpu.VMEM),
            scratch_shapes=[
                pltpu.VMEM((4, 10, 128, 128), BF16),
                pltpu.VMEM((3, 3, 384, 128), BF16),
                pltpu.VMEM((3, 384, 256), BF16),
                pltpu.VMEM((3, 3, 768, 256), BF16),
                pltpu.VMEM((2, 8, 128, 128), F32),
                pltpu.VMEM((9, 136, 128), F32),
                pltpu.VMEM((2, 128, 128), BF16),
                pltpu.VMEM((3, 6, 64, 256), BF16),
                pltpu.VMEM((3, 256, 256), F32),
                pltpu.SemaphoreType.DMA((len(IDS),)),
                pltpu.SemaphoreType.DMA((len(IDS),)),
                pltpu.SemaphoreType.DMA((4,)),
            ],
            compiler_params=pltpu.CompilerParams(
                collective_id=0, has_side_effects=True, vmem_limit_bytes=60 * 1024 * 1024
            ),
            name="encoder",
        )(frames, conv_fine, conv_down, conv_coarse)

    placed = (P("tm", "rows", None, None), P(), P(), P())
    return jax.shard_map(
        local, mesh=mesh, in_specs=placed, out_specs=P("tm", "rows", None, None), check_vma=False
    )
```

```python
import jax
import jax.numpy as jnp
from jax import lax
from jax.experimental import pallas as pl
from jax.experimental.pallas import tpu as pltpu
from jax.sharding import PartitionSpec as P

MESH = pl.DeviceIdType.MESH
F32 = jnp.float32
BF16 = jnp.bfloat16

NAMES = (
    "E0", "E1", "S0", "M0", "M1", "OU", "OD", "FU", "FD", "HU", "HD", "PR",
    "N0", "N1", "N2", "N3", "Q0", "Q1", "Q2", "Q3", "G0", "G1", "G2", "G3",
    "T2U", "T2D", "T1U", "T1D", "T0U", "T0D", "K0U", "K0D",
)
IDS = {name: i for i, name in enumerate(NAMES)}


def silu(v):
    return v / (1.0 + jnp.exp(-v))


def spread(y0, y1, y2, cols):
    col = lax.broadcasted_iota(jnp.int32, y0.shape, 0) % cols
    left = jnp.where(col == 0, 0.0, pltpu.roll(y0, 1, 0))
    right = jnp.where(col == cols - 1, 0.0, pltpu.roll(y2, y2.shape[0] - 1, 0))
    return left + y1 + right


def dot(a, b):
    return jnp.dot(a, b, preferred_element_type=F32)


def kernel(
    tms, rws, frames, wf_h, wd_h, wc_h, out, x, wf, wd, wc, z, pool, rim, red, y, ssem, rsem, lsem, near
):
    tm = lax.axis_index("tm")
    row = lax.axis_index("rows")
    first = tm % 2 == 0
    second = ~first
    has_next, has_prev = tm < tms - 1, tm > 0
    has_next2, has_prev2 = tm < tms - 2, tm > 1
    up, down = row > 0, row < rws - 1
    half = rws // 2
    cross_up, cross_down = row == half, row == half - 1

    barrier = pltpu.get_barrier_semaphore()
    total = jnp.int32(0)
    for ok, dev in (
        (has_next, (tm + 1, row)),
        (has_prev, (tm - 1, row)),
        (up, (tm, row - 1)),
        (down, (tm, row + 1)),
        (first & has_next2, (tm + 2, row)),
        (first & has_prev2, (tm - 2, row)),
        (second & has_next & cross_up, (tm + 1, row - 1)),
        (second & has_next & cross_down, (tm + 1, row + 1)),
        (first & has_prev & cross_up, (tm - 1, row - 1)),
        (first & has_prev & cross_down, (tm - 1, row + 1)),
    ):

        @pl.when(ok)
        def _():
            pl.semaphore_signal(barrier, inc=1, device_id=dev, device_id_type=MESH)

        total = total + ok.astype(jnp.int32)

    loads = [
        pltpu.make_async_copy(frames, x.at[pl.ds(2, 2), pl.ds(1, 8)], lsem.at[0]),
        pltpu.make_async_copy(wf_h, wf, lsem.at[1]),
        pltpu.make_async_copy(wd_h, wd, lsem.at[2]),
        pltpu.make_async_copy(wc_h, wc, lsem.at[3]),
    ]
    for load in loads:
        load.start()

    pool[:, pl.ds(128, 8), :] = jnp.zeros((9, 8, 128), F32)

    @pl.when(~up)
    def _():
        x[:, 0] = jnp.zeros((4, 128, 128), BF16)
        red[:, 0] = jnp.zeros((3, 64, 256), BF16)

    @pl.when(~down)
    def _():
        x[:, 9] = jnp.zeros((4, 128, 128), BF16)
        red[:, 5] = jnp.zeros((3, 64, 256), BF16)
        rim[1] = jnp.zeros((128, 128), BF16)

    @pl.when(~has_prev)
    def _():
        x[0:2, pl.ds(1, 8)] = jnp.zeros((2, 8, 128, 128), BF16)
        red[1, pl.ds(1, 4)] = jnp.zeros((4, 64, 256), BF16)

        @pl.when(up)
        def _():
            x[0:2, 0] = jnp.zeros((2, 128, 128), BF16)
            red[1, 0] = jnp.zeros((64, 256), BF16)

        @pl.when(down)
        def _():
            x[0:2, 9] = jnp.zeros((2, 128, 128), BF16)
            red[1, 5] = jnp.zeros((64, 256), BF16)

    @pl.when(~has_prev2)
    def _():
        red[0, pl.ds(1, 4)] = jnp.zeros((4, 64, 256), BF16)

        @pl.when(up)
        def _():
            red[0, 0] = jnp.zeros((64, 256), BF16)

        @pl.when(down)
        def _():
            red[0, 5] = jnp.zeros((64, 256), BF16)

    sent = []

    def send(ok, name, src, dst, dev, recv=None):
        copy = pltpu.make_async_remote_copy(
            src_ref=src,
            dst_ref=dst,
            send_sem=ssem.at[IDS[name]],
            recv_sem=rsem.at[IDS[recv or name]],
            device_id=dev,
            device_id_type=MESH,
        )

        @pl.when(ok)
        def _():
            copy.start()

        sent.append((ok, copy))

    def left(ok):
        for i, (was, copy) in enumerate(sent):

            @pl.when(was & ok)
            def _():
                copy.wait_send()

            sent[i] = (was & ~ok, copy)

    def arrived(ok, name, dst):
        copy = pltpu.make_async_remote_copy(
            src_ref=dst,
            dst_ref=dst,
            send_sem=ssem.at[IDS[name]],
            recv_sem=rsem.at[IDS[name]],
            device_id=nxt,
            device_id_type=MESH,
        )

        @pl.when(ok)
        def _():
            copy.wait_recv()

    nxt, nx2 = (tm + 1, row), (tm + 2, row)
    above, below = (tm, row - 1), (tm, row + 1)

    def own(r, n=1):
        return x.at[pl.ds(2, 2), pl.ds(r, n)]

    def old(r, n=1):
        return x.at[pl.ds(0, 2), pl.ds(r, n)]

    def part(a, r, n=1):
        return red.at[a, pl.ds(r, n)]

    def tap(a, b, e):
        return wf[a, b, pl.ds(e * 128, 128), :]

    def fine(lhs, main, side, both, single, other):
        left = jnp.concatenate(
            [lhs(main, b) for b in range(3)] + [lhs(side, b) for b in range(3)], axis=1
        )

        def rhs(pairs):
            return jnp.concatenate([jnp.concatenate(pair, axis=1) for pair in pairs], axis=0)

        none = jnp.zeros((128, 128), BF16)
        n0 = dot(
            left,
            rhs(
                [(tap(both, b, 0), tap(both, b, 1)) for b in range(3)]
                + [(tap(single, b, 0), tap(single, b, 1)) for b in range(3)]
            ),
        )
        n1 = dot(
            left,
            rhs(
                [(tap(both, b, 2), tap(other, b, 0)) for b in range(3)]
                + [(tap(single, b, 2), none) for b in range(3)]
            ),
        )
        n2 = dot(left[:, :384], rhs([(tap(other, b, 1), tap(other, b, 2)) for b in range(3)]))
        mine = spread(n0[:, :128], n0[:, 128:], n1[:, :128], 128)
        rest = spread(n1[:, 128:], n2[:, :128], n2[:, 128:], 128)
        return mine, rest

    def late(lhs):
        second, head = fine(lhs, 2, 3, 1, 2, 2)
        return head, second

    def early(lhs):
        return fine(lhs, 1, 0, 1, 0, 0)

    def pooled(head, second):
        a = silu(head).astype(BF16).astype(F32)
        b = silu(second).astype(BF16).astype(F32)
        return ((a + b) * 0.5).astype(BF16).astype(F32)

    def inner(r):
        return lambda f, b: x[f, pl.ds(r + b, 2)].reshape(256, 128)

    loads[0].wait()
    loads[1].wait()

    def own_part(i, carry):
        r = 2 * i + 1
        head, second = late(inner(r))
        z[0, pl.ds(r, 2)] = head.reshape(2, 128, 128)
        z[1, pl.ds(r, 2)] = second.reshape(2, 128, 128)
        return carry

    lax.fori_loop(0, 3, own_part, 0)
    pl.semaphore_wait(barrier, total)

    @pl.when(has_prev)
    def _():
        pl.semaphore_signal(near, inc=1, device_id=(tm - 1, row), device_id_type=MESH)

    @pl.when(first & has_prev2)
    def _():
        pl.semaphore_signal(near, inc=1, device_id=(tm - 2, row), device_id_type=MESH)

    far = first & has_prev
    lead = second & has_next
    send(up, "OU", own(1), own(9), above)
    send(down, "OD", own(8), own(0), below)
    send(lead & cross_up, "FU", own(1), old(9), (tm + 1, row - 1))
    send(lead & cross_down, "FD", own(8), old(0), (tm + 1, row + 1))
    left(lead & (cross_up | cross_down))
    send(has_next, "E1", own(8), old(8), nxt)
    send(has_next, "E0", own(1), old(1), nxt)
    send(has_next, "S0", own(2), old(2), nxt)
    send(has_next, "M0", own(3, 2), old(3, 2), nxt)
    send(has_next, "M1", own(5, 3), old(5, 3), nxt)

    arrived(down, "OU", own(9))
    send(first & down, "HU", own(9), old(9), nxt, "FU")
    arrived(up, "OD", own(0))
    send(first & up, "HD", own(0), old(0), nxt, "FD")
    arrived(has_prev, "E1", old(8))
    send(far & down & ~cross_down, "FD", old(8), old(0), below)
    arrived(has_prev, "E0", old(1))
    send(far & up & ~cross_up, "FU", old(1), old(9), above)

    head_a, second_a = late(lambda f, b: jnp.concatenate([x[f, b], x[f, 7 + b]], axis=0))
    z[0, 7] = head_a[128:]
    z[1, 7] = second_a[128:]
    arrived(up & has_prev, "FD", old(0))
    arrived(has_prev, "S0", old(2))
    head_b, second_b = early(lambda f, b: x[f, b])
    top = pooled(head_a[:128] + head_b, second_a[:128] + second_b)
    pool[0, pl.ds(0, 128)] = top
    rim[0] = top.astype(BF16)
    send(up, "PR", rim.at[0], rim.at[1], above)

    def rest_part(i, carry):
        r = 2 * i + 1
        head, second = early(inner(r))
        head = head + z[0, pl.ds(r, 2)].reshape(256, 128)
        second = second + z[1, pl.ds(r, 2)].reshape(256, 128)
        pool[pl.ds(r, 2), pl.ds(0, 128)] = pooled(head, second).reshape(2, 128, 128)
        return carry

    def reduce(p):
        strip = [
            pool[2 * p + b, pl.ds(e, 64, stride=2), :].astype(BF16)
            for b in range(3)
            for e in range(3)
        ]
        red[2, p + 1] = dot(jnp.concatenate(strip, axis=1), wd[...].reshape(1152, 256)).astype(BF16)

    hop2 = first & has_next2

    def pass_on(p):
        send(has_next, "N%d" % p, part(2, p + 1), part(1, p + 1), nxt)
        send(hop2, "Q%d" % p, part(2, p + 1), part(0, p + 1), nx2)

    def rim_up():
        send(up, "T2U", part(2, 1), part(2, 5), above)
        send(up & has_next, "T1U", part(2, 1), part(1, 5), (tm + 1, row - 1))
        send(up & hop2, "T0U", part(2, 1), part(0, 5), (tm + 2, row - 1))

    def rim_down():
        send(down, "T2D", part(2, 4), part(2, 0), below)
        send(down & has_next, "T1D", part(2, 4), part(1, 0), (tm + 1, row + 1))
        send(down & hop2, "T0D", part(2, 4), part(0, 0), (tm + 2, row + 1))

    loads[2].wait()

    @pl.when(has_next)
    def _():
        pl.semaphore_wait(near, 1 + hop2.astype(jnp.int32))

    arrived(has_prev, "M0", old(3, 2))
    rest_part(0, 0)
    reduce(0)
    rim_up()
    pass_on(0)
    arrived(has_prev, "M1", old(5, 3))
    rest_part(1, 0)
    reduce(1)
    pass_on(1)
    rest_part(2, 0)
    reduce(2)
    pass_on(2)
    arrived(down & has_prev, "FU", old(9))
    head_b, second_b = early(lambda f, b: x[f, 7 + b])
    pool[7, pl.ds(0, 128)] = pooled(z[0, 7] + head_b, z[1, 7] + second_b)
    arrived(down, "PR", rim.at[1])
    pool[8, pl.ds(0, 128)] = rim[1].astype(F32)
    reduce(3)
    rim_down()
    pass_on(3)

    def coarse(a, e):
        left = jnp.concatenate(
            [red[a, pl.ds(b, 4)].reshape(256, 256) for b in range(3)], axis=1
        )
        right = jnp.concatenate([wc[a, b, pl.ds(e * 256, 256), :] for b in range(3)], axis=0)
        return dot(left, right)

    loads[3].wait()
    for p in range(3):
        arrived(has_prev, "N%d" % p, part(1, p + 1))
        send(far, "G%d" % p, part(1, p + 1), part(0, p + 1), nxt, "Q%d" % p)
    arrived(down & has_prev, "T1U", part(1, 5))
    send(far & down, "K0U", part(1, 5), part(0, 5), nxt, "T0U")
    arrived(down, "T2U", part(2, 5))
    arrived(up, "T2D", part(2, 0))
    for e in range(3):
        y[e] = coarse(2, e)
    arrived(has_prev, "N3", part(1, 4))
    send(far, "G3", part(1, 4), part(0, 4), nxt, "Q3")
    arrived(up & has_prev, "T1D", part(1, 0))
    send(far & up, "K0D", part(1, 0), part(0, 0), nxt, "T0D")
    for e in range(3):
        y[e] = y[e] + coarse(1, e)
    for p in range(4):
        arrived(has_prev2, "Q%d" % p, part(0, p + 1))
    arrived(down & has_prev2, "T0U", part(0, 5))
    arrived(up & has_prev2, "T0D", part(0, 0))
    parts = [y[e] + coarse(0, e) for e in range(3)]
    out[...] = silu(spread(*parts, 64)).astype(BF16).reshape(1, 4, 64, 256)

    for ok, copy in sent:

        @pl.when(ok)
        def _():
            copy.wait_send()


def solution(mesh):
    import functools

    tms, rws = mesh.shape["tm"], mesh.shape["rows"]
    anywhere = pl.BlockSpec(memory_space=pl.ANY)

    def local(frames, conv_fine, conv_down, conv_coarse):
        return pl.pallas_call(
            functools.partial(kernel, tms, rws),
            out_shape=jax.ShapeDtypeStruct((1, 4, 64, 256), BF16),
            in_specs=[anywhere] * 4,
            out_specs=pl.BlockSpec(memory_space=pltpu.VMEM),
            scratch_shapes=[
                pltpu.VMEM((4, 10, 128, 128), BF16),
                pltpu.VMEM((3, 3, 384, 128), BF16),
                pltpu.VMEM((3, 384, 256), BF16),
                pltpu.VMEM((3, 3, 768, 256), BF16),
                pltpu.VMEM((2, 8, 128, 128), F32),
                pltpu.VMEM((9, 136, 128), F32),
                pltpu.VMEM((2, 128, 128), BF16),
                pltpu.VMEM((3, 6, 64, 256), BF16),
                pltpu.VMEM((3, 256, 256), F32),
                pltpu.SemaphoreType.DMA((len(IDS),)),
                pltpu.SemaphoreType.DMA((len(IDS),)),
                pltpu.SemaphoreType.DMA((4,)),
                pltpu.SemaphoreType.REGULAR,
            ],
            compiler_params=pltpu.CompilerParams(
                collective_id=0, has_side_effects=True, vmem_limit_bytes=60 * 1024 * 1024
            ),
            name="encoder",
        )(frames, conv_fine, conv_down, conv_coarse)

    placed = (P("tm", "rows", None, None), P(), P(), P())
    return jax.shard_map(
        local, mesh=mesh, in_specs=placed, out_specs=P("tm", "rows", None, None), check_vma=False
    )
```

```python
import jax
import jax.numpy as jnp
from jax import lax
from jax.experimental import pallas as pl
from jax.experimental.pallas import tpu as pltpu
from jax.sharding import PartitionSpec as P

MESH = pl.DeviceIdType.MESH
F32 = jnp.float32
BF16 = jnp.bfloat16

NAMES = (
    "E0", "E1", "S0", "M0", "M1", "OU", "OD", "FU", "FD", "HU", "HD", "PR",
    "N0", "N1", "N2", "N3", "Q0", "Q1", "Q2", "Q3", "G0", "G1", "G2", "G3",
    "T2U", "T2D", "T1U", "T1D", "T0U", "T0D", "K0U", "K0D",
)
IDS = {name: i for i, name in enumerate(NAMES)}


def silu(v):
    return v / (1.0 + jnp.exp(-v))


def spread(y0, y1, y2, cols):
    col = lax.broadcasted_iota(jnp.int32, y0.shape, 0) % cols
    left = jnp.where(col == 0, 0.0, pltpu.roll(y0, 1, 0))
    right = jnp.where(col == cols - 1, 0.0, pltpu.roll(y2, y2.shape[0] - 1, 0))
    return left + y1 + right


def dot(a, b):
    return jnp.dot(a, b, preferred_element_type=F32)


def kernel(
    tms, rws, frames, wf_h, wd_h, wc_h, out, x, wf, wd, wc, z, pool, rim, red, y, ssem, rsem, lsem, near
):
    tm = lax.axis_index("tm")
    row = lax.axis_index("rows")
    first = tm % 2 == 0
    second = ~first
    has_next, has_prev = tm < tms - 1, tm > 0
    has_next2, has_prev2 = tm < tms - 2, tm > 1
    up, down = row > 0, row < rws - 1
    half = rws // 2
    cross_up, cross_down = row == half, row == half - 1

    barrier = pltpu.get_barrier_semaphore()
    total = jnp.int32(0)
    for ok, dev in (
        (has_next, (tm + 1, row)),
        (has_prev, (tm - 1, row)),
        (up, (tm, row - 1)),
        (down, (tm, row + 1)),
        (first & has_next2, (tm + 2, row)),
        (first & has_prev2, (tm - 2, row)),
    ):

        @pl.when(ok)
        def _():
            pl.semaphore_signal(barrier, inc=1, device_id=dev, device_id_type=MESH)

        total = total + ok.astype(jnp.int32)

    loads = [
        pltpu.make_async_copy(frames, x.at[pl.ds(2, 2), pl.ds(1, 8)], lsem.at[0]),
        pltpu.make_async_copy(wf_h, wf, lsem.at[1]),
        pltpu.make_async_copy(wd_h, wd, lsem.at[2]),
        pltpu.make_async_copy(wc_h, wc, lsem.at[3]),
    ]
    for load in loads:
        load.start()

    pool[:, pl.ds(128, 8), :] = jnp.zeros((9, 8, 128), F32)

    @pl.when(~up)
    def _():
        x[:, 0] = jnp.zeros((4, 128, 128), BF16)
        red[:, 0] = jnp.zeros((3, 64, 256), BF16)

    @pl.when(~down)
    def _():
        x[:, 9] = jnp.zeros((4, 128, 128), BF16)
        red[:, 5] = jnp.zeros((3, 64, 256), BF16)
        rim[1] = jnp.zeros((128, 128), BF16)

    @pl.when(~has_prev)
    def _():
        x[0:2, pl.ds(1, 8)] = jnp.zeros((2, 8, 128, 128), BF16)
        red[1, pl.ds(1, 4)] = jnp.zeros((4, 64, 256), BF16)

        @pl.when(up)
        def _():
            x[0:2, 0] = jnp.zeros((2, 128, 128), BF16)
            red[1, 0] = jnp.zeros((64, 256), BF16)

        @pl.when(down)
        def _():
            x[0:2, 9] = jnp.zeros((2, 128, 128), BF16)
            red[1, 5] = jnp.zeros((64, 256), BF16)

    @pl.when(~has_prev2)
    def _():
        red[0, pl.ds(1, 4)] = jnp.zeros((4, 64, 256), BF16)

        @pl.when(up)
        def _():
            red[0, 0] = jnp.zeros((64, 256), BF16)

        @pl.when(down)
        def _():
            red[0, 5] = jnp.zeros((64, 256), BF16)

    sent = []

    def send(ok, name, src, dst, dev, recv=None):
        copy = pltpu.make_async_remote_copy(
            src_ref=src,
            dst_ref=dst,
            send_sem=ssem.at[IDS[name]],
            recv_sem=rsem.at[IDS[recv or name]],
            device_id=dev,
            device_id_type=MESH,
        )

        @pl.when(ok)
        def _():
            copy.start()

        sent.append((ok, copy))

    def arrived(ok, name, dst):
        copy = pltpu.make_async_remote_copy(
            src_ref=dst,
            dst_ref=dst,
            send_sem=ssem.at[IDS[name]],
            recv_sem=rsem.at[IDS[name]],
            device_id=nxt,
            device_id_type=MESH,
        )

        @pl.when(ok)
        def _():
            copy.wait_recv()

    nxt, nx2 = (tm + 1, row), (tm + 2, row)
    above, below = (tm, row - 1), (tm, row + 1)

    def own(r, n=1):
        return x.at[pl.ds(2, 2), pl.ds(r, n)]

    def old(r, n=1):
        return x.at[pl.ds(0, 2), pl.ds(r, n)]

    def part(a, r, n=1):
        return red.at[a, pl.ds(r, n)]

    def tap(a, b, e):
        return wf[a, b, pl.ds(e * 128, 128), :]

    def fine(lhs, main, side, both, single, other):
        left = jnp.concatenate(
            [lhs(main, b) for b in range(3)] + [lhs(side, b) for b in range(3)], axis=1
        )

        def rhs(pairs):
            return jnp.concatenate([jnp.concatenate(pair, axis=1) for pair in pairs], axis=0)

        none = jnp.zeros((128, 128), BF16)
        n0 = dot(
            left,
            rhs(
                [(tap(both, b, 0), tap(both, b, 1)) for b in range(3)]
                + [(tap(single, b, 0), tap(single, b, 1)) for b in range(3)]
            ),
        )
        n1 = dot(
            left,
            rhs(
                [(tap(both, b, 2), tap(other, b, 0)) for b in range(3)]
                + [(tap(single, b, 2), none) for b in range(3)]
            ),
        )
        n2 = dot(left[:, :384], rhs([(tap(other, b, 1), tap(other, b, 2)) for b in range(3)]))
        mine = spread(n0[:, :128], n0[:, 128:], n1[:, :128], 128)
        rest = spread(n1[:, 128:], n2[:, :128], n2[:, 128:], 128)
        return mine, rest

    def late(lhs):
        second, head = fine(lhs, 2, 3, 1, 2, 2)
        return head, second

    def early(lhs):
        return fine(lhs, 1, 0, 1, 0, 0)

    def pooled(head, second):
        a = silu(head).astype(BF16).astype(F32)
        b = silu(second).astype(BF16).astype(F32)
        return ((a + b) * 0.5).astype(BF16).astype(F32)

    def inner(r):
        return lambda f, b: x[f, pl.ds(r + b, 2)].reshape(256, 128)

    loads[0].wait()
    loads[1].wait()

    def own_part(i, carry):
        r = 2 * i + 1
        head, second = late(inner(r))
        z[0, pl.ds(r, 2)] = head.reshape(2, 128, 128)
        z[1, pl.ds(r, 2)] = second.reshape(2, 128, 128)
        return carry

    lax.fori_loop(0, 3, own_part, 0)
    pl.semaphore_wait(barrier, total)

    @pl.when(has_prev)
    def _():
        pl.semaphore_signal(near, inc=1, device_id=(tm - 1, row), device_id_type=MESH)

    @pl.when(first & has_prev2)
    def _():
        pl.semaphore_signal(near, inc=1, device_id=(tm - 2, row), device_id_type=MESH)

    far = first & has_prev
    lead = second & has_next
    send(up, "OU", own(1), own(9), above)
    send(down, "OD", own(8), own(0), below)
    hold = second & ((tm // 2) % 2 == 1)
    arrived(hold & cross_down, "OU", own(9))
    arrived(hold & cross_up, "OD", own(0))
    send(has_next, "E1", own(8), old(8), nxt)
    send(has_next, "E0", own(1), old(1), nxt)
    send(has_next, "S0", own(2), old(2), nxt)
    send(has_next, "M0", own(3, 2), old(3, 2), nxt)
    arrived(second & ~hold & cross_down, "OU", own(9))
    arrived(second & ~hold & cross_up, "OD", own(0))
    send(lead & cross_down, "HU", own(9), old(9), nxt, "FU")
    send(lead & cross_up, "HD", own(0), old(0), nxt, "FD")
    send(has_next, "M1", own(5, 3), old(5, 3), nxt)

    arrived(down & ~(second & cross_down), "OU", own(9))
    send(first & down, "HU", own(9), old(9), nxt, "FU")
    arrived(up & ~(second & cross_up), "OD", own(0))
    send(first & up, "HD", own(0), old(0), nxt, "FD")
    arrived(has_prev, "E1", old(8))
    send(far & down & ~cross_down, "FD", old(8), old(0), below)
    arrived(has_prev, "E0", old(1))
    send(far & up & ~cross_up, "FU", old(1), old(9), above)

    head_a, second_a = late(lambda f, b: jnp.concatenate([x[f, b], x[f, 7 + b]], axis=0))
    z[0, 7] = head_a[128:]
    z[1, 7] = second_a[128:]
    arrived(up & has_prev, "FD", old(0))
    arrived(has_prev, "S0", old(2))
    head_b, second_b = early(lambda f, b: x[f, b])
    top = pooled(head_a[:128] + head_b, second_a[:128] + second_b)
    pool[0, pl.ds(0, 128)] = top
    rim[0] = top.astype(BF16)
    send(up, "PR", rim.at[0], rim.at[1], above)

    def rest_part(i, carry):
        r = 2 * i + 1
        head, second = early(inner(r))
        head = head + z[0, pl.ds(r, 2)].reshape(256, 128)
        second = second + z[1, pl.ds(r, 2)].reshape(256, 128)
        pool[pl.ds(r, 2), pl.ds(0, 128)] = pooled(head, second).reshape(2, 128, 128)
        return carry

    def reduce(p):
        strip = [
            pool[2 * p + b, pl.ds(e, 64, stride=2), :].astype(BF16)
            for b in range(3)
            for e in range(3)
        ]
        red[2, p + 1] = dot(jnp.concatenate(strip, axis=1), wd[...].reshape(1152, 256)).astype(BF16)

    hop2 = first & has_next2

    def pass_on(p):
        send(has_next, "N%d" % p, part(2, p + 1), part(1, p + 1), nxt)
        send(hop2, "Q%d" % p, part(2, p + 1), part(0, p + 1), nx2)

    def rim_up():
        send(up, "T2U", part(2, 1), part(2, 5), above)
        send(up & has_next, "T1U", part(2, 1), part(1, 5), (tm + 1, row - 1))
        send(up & hop2, "T0U", part(2, 1), part(0, 5), (tm + 2, row - 1))

    def rim_down():
        send(down, "T2D", part(2, 4), part(2, 0), below)
        send(down & has_next, "T1D", part(2, 4), part(1, 0), (tm + 1, row + 1))
        send(down & hop2, "T0D", part(2, 4), part(0, 0), (tm + 2, row + 1))

    loads[2].wait()

    @pl.when(has_next)
    def _():
        pl.semaphore_wait(near, 1 + hop2.astype(jnp.int32))

    arrived(has_prev, "M0", old(3, 2))
    rest_part(0, 0)
    reduce(0)
    rim_up()
    pass_on(0)
    arrived(has_prev, "M1", old(5, 3))
    rest_part(1, 0)
    reduce(1)
    pass_on(1)
    rest_part(2, 0)
    reduce(2)
    pass_on(2)
    arrived(down & has_prev, "FU", old(9))
    head_b, second_b = early(lambda f, b: x[f, 7 + b])
    pool[7, pl.ds(0, 128)] = pooled(z[0, 7] + head_b, z[1, 7] + second_b)
    arrived(down, "PR", rim.at[1])
    pool[8, pl.ds(0, 128)] = rim[1].astype(F32)
    reduce(3)
    rim_down()
    pass_on(3)

    def coarse(a, e):
        left = jnp.concatenate(
            [red[a, pl.ds(b, 4)].reshape(256, 256) for b in range(3)], axis=1
        )
        right = jnp.concatenate([wc[a, b, pl.ds(e * 256, 256), :] for b in range(3)], axis=0)
        return dot(left, right)

    loads[3].wait()
    for p in range(3):
        arrived(has_prev, "N%d" % p, part(1, p + 1))
        send(far, "G%d" % p, part(1, p + 1), part(0, p + 1), nxt, "Q%d" % p)
    arrived(down & has_prev, "T1U", part(1, 5))
    send(far & down, "K0U", part(1, 5), part(0, 5), nxt, "T0U")
    arrived(down, "T2U", part(2, 5))
    arrived(up, "T2D", part(2, 0))
    for e in range(3):
        y[e] = coarse(2, e)
    arrived(has_prev, "N3", part(1, 4))
    send(far, "G3", part(1, 4), part(0, 4), nxt, "Q3")
    arrived(up & has_prev, "T1D", part(1, 0))
    send(far & up, "K0D", part(1, 0), part(0, 0), nxt, "T0D")
    for e in range(3):
        y[e] = y[e] + coarse(1, e)
    for p in range(4):
        arrived(has_prev2, "Q%d" % p, part(0, p + 1))
    arrived(down & has_prev2, "T0U", part(0, 5))
    arrived(up & has_prev2, "T0D", part(0, 0))
    parts = [y[e] + coarse(0, e) for e in range(3)]
    out[...] = silu(spread(*parts, 64)).astype(BF16).reshape(1, 4, 64, 256)

    for ok, copy in sent:

        @pl.when(ok)
        def _():
            copy.wait_send()


def solution(mesh):
    import functools

    tms, rws = mesh.shape["tm"], mesh.shape["rows"]
    anywhere = pl.BlockSpec(memory_space=pl.ANY)

    def local(frames, conv_fine, conv_down, conv_coarse):
        return pl.pallas_call(
            functools.partial(kernel, tms, rws),
            out_shape=jax.ShapeDtypeStruct((1, 4, 64, 256), BF16),
            in_specs=[anywhere] * 4,
            out_specs=pl.BlockSpec(memory_space=pltpu.VMEM),
            scratch_shapes=[
                pltpu.VMEM((4, 10, 128, 128), BF16),
                pltpu.VMEM((3, 3, 384, 128), BF16),
                pltpu.VMEM((3, 384, 256), BF16),
                pltpu.VMEM((3, 3, 768, 256), BF16),
                pltpu.VMEM((2, 8, 128, 128), F32),
                pltpu.VMEM((9, 136, 128), F32),
                pltpu.VMEM((2, 128, 128), BF16),
                pltpu.VMEM((3, 6, 64, 256), BF16),
                pltpu.VMEM((3, 256, 256), F32),
                pltpu.SemaphoreType.DMA((len(IDS),)),
                pltpu.SemaphoreType.DMA((len(IDS),)),
                pltpu.SemaphoreType.DMA((4,)),
                pltpu.SemaphoreType.REGULAR,
            ],
            compiler_params=pltpu.CompilerParams(
                collective_id=0, has_side_effects=True, vmem_limit_bytes=60 * 1024 * 1024
            ),
            name="encoder",
        )(frames, conv_fine, conv_down, conv_coarse)

    placed = (P("tm", "rows", None, None), P(), P(), P())
    return jax.shard_map(
        local, mesh=mesh, in_specs=placed, out_specs=P("tm", "rows", None, None), check_vma=False
    )
```

```python
import jax
import jax.numpy as jnp
from jax import lax
from jax.experimental import pallas as pl
from jax.experimental.pallas import tpu as pltpu
from jax.sharding import PartitionSpec as P

MESH = pl.DeviceIdType.MESH
F32 = jnp.float32
BF16 = jnp.bfloat16

NAMES = (
    "E0", "E1", "S0", "M0", "M1", "OU", "OD", "FU", "FD", "HU", "HD", "PR",
    "N0", "N1", "N2", "N3", "Q0", "Q1", "Q2", "Q3", "G0", "G1", "G2", "G3",
    "T2U", "T2D", "T1U", "T1D", "T0U", "T0D", "K0U", "K0D",
)
IDS = {name: i for i, name in enumerate(NAMES)}


def silu(v):
    return v / (1.0 + jnp.exp(-v))


def spread(y0, y1, y2, cols):
    col = lax.broadcasted_iota(jnp.int32, y0.shape, 0) % cols
    left = jnp.where(col == 0, 0.0, pltpu.roll(y0, 1, 0))
    right = jnp.where(col == cols - 1, 0.0, pltpu.roll(y2, y2.shape[0] - 1, 0))
    return left + y1 + right


def dot(a, b):
    return jnp.dot(a, b, preferred_element_type=F32)


def kernel(
    tms, rws, frames, wf_h, wd_h, wc_h, out, x, wf, wd, wc, z, pool, rim, red, y, ssem, rsem, lsem, near
):
    tm = lax.axis_index("tm")
    row = lax.axis_index("rows")
    first = tm % 2 == 0
    second = ~first
    has_next, has_prev = tm < tms - 1, tm > 0
    has_next2, has_prev2 = tm < tms - 2, tm > 1
    up, down = row > 0, row < rws - 1
    half = rws // 2
    cross_up, cross_down = row == half, row == half - 1

    barrier = pltpu.get_barrier_semaphore()
    total = jnp.int32(0)
    for ok, dev in (
        (has_next, (tm + 1, row)),
        (has_prev, (tm - 1, row)),
        (up, (tm, row - 1)),
        (down, (tm, row + 1)),
        (first & has_next2, (tm + 2, row)),
        (first & has_prev2, (tm - 2, row)),
    ):

        @pl.when(ok)
        def _():
            pl.semaphore_signal(barrier, inc=1, device_id=dev, device_id_type=MESH)

        total = total + ok.astype(jnp.int32)

    loads = [
        pltpu.make_async_copy(frames, x.at[pl.ds(2, 2), pl.ds(1, 8)], lsem.at[0]),
        pltpu.make_async_copy(wf_h, wf, lsem.at[1]),
        pltpu.make_async_copy(wd_h, wd, lsem.at[2]),
        pltpu.make_async_copy(wc_h, wc, lsem.at[3]),
    ]
    for load in loads:
        load.start()

    pool[:, pl.ds(128, 8), :] = jnp.zeros((9, 8, 128), F32)

    @pl.when(~up)
    def _():
        x[:, 0] = jnp.zeros((4, 128, 128), BF16)
        red[:, 0] = jnp.zeros((3, 64, 256), BF16)

    @pl.when(~down)
    def _():
        x[:, 9] = jnp.zeros((4, 128, 128), BF16)
        red[:, 5] = jnp.zeros((3, 64, 256), BF16)
        rim[1] = jnp.zeros((128, 128), BF16)

    @pl.when(~has_prev)
    def _():
        x[0:2, pl.ds(1, 8)] = jnp.zeros((2, 8, 128, 128), BF16)
        red[1, pl.ds(1, 4)] = jnp.zeros((4, 64, 256), BF16)

        @pl.when(up)
        def _():
            x[0:2, 0] = jnp.zeros((2, 128, 128), BF16)
            red[1, 0] = jnp.zeros((64, 256), BF16)

        @pl.when(down)
        def _():
            x[0:2, 9] = jnp.zeros((2, 128, 128), BF16)
            red[1, 5] = jnp.zeros((64, 256), BF16)

    @pl.when(~has_prev2)
    def _():
        red[0, pl.ds(1, 4)] = jnp.zeros((4, 64, 256), BF16)

        @pl.when(up)
        def _():
            red[0, 0] = jnp.zeros((64, 256), BF16)

        @pl.when(down)
        def _():
            red[0, 5] = jnp.zeros((64, 256), BF16)

    sent = []

    def send(ok, name, src, dst, dev, recv=None):
        copy = pltpu.make_async_remote_copy(
            src_ref=src,
            dst_ref=dst,
            send_sem=ssem.at[IDS[name]],
            recv_sem=rsem.at[IDS[recv or name]],
            device_id=dev,
            device_id_type=MESH,
        )

        @pl.when(ok)
        def _():
            copy.start()

        sent.append((ok, copy))

    def arrived(ok, name, dst):
        copy = pltpu.make_async_remote_copy(
            src_ref=dst,
            dst_ref=dst,
            send_sem=ssem.at[IDS[name]],
            recv_sem=rsem.at[IDS[name]],
            device_id=nxt,
            device_id_type=MESH,
        )

        @pl.when(ok)
        def _():
            copy.wait_recv()

    nxt, nx2 = (tm + 1, row), (tm + 2, row)
    above, below = (tm, row - 1), (tm, row + 1)

    def own(r, n=1):
        return x.at[pl.ds(2, 2), pl.ds(r, n)]

    def old(r, n=1):
        return x.at[pl.ds(0, 2), pl.ds(r, n)]

    def part(a, r, n=1):
        return red.at[a, pl.ds(r, n)]

    def tap(a, b, e):
        return wf[a, b, pl.ds(e * 128, 128), :]

    def fine(lhs, main, side, both, single, other):
        left = jnp.concatenate(
            [lhs(main, b) for b in range(3)] + [lhs(side, b) for b in range(3)], axis=1
        )

        def rhs(pairs):
            return jnp.concatenate([jnp.concatenate(pair, axis=1) for pair in pairs], axis=0)

        none = jnp.zeros((128, 128), BF16)
        n0 = dot(
            left,
            rhs(
                [(tap(both, b, 0), tap(both, b, 1)) for b in range(3)]
                + [(tap(single, b, 0), tap(single, b, 1)) for b in range(3)]
            ),
        )
        n1 = dot(
            left,
            rhs(
                [(tap(both, b, 2), tap(other, b, 0)) for b in range(3)]
                + [(tap(single, b, 2), none) for b in range(3)]
            ),
        )
        n2 = dot(left[:, :384], rhs([(tap(other, b, 1), tap(other, b, 2)) for b in range(3)]))
        mine = spread(n0[:, :128], n0[:, 128:], n1[:, :128], 128)
        rest = spread(n1[:, 128:], n2[:, :128], n2[:, 128:], 128)
        return mine, rest

    def late(lhs):
        second, head = fine(lhs, 2, 3, 1, 2, 2)
        return head, second

    def early(lhs):
        return fine(lhs, 1, 0, 1, 0, 0)

    def pooled(head, second):
        a = silu(head).astype(BF16).astype(F32)
        b = silu(second).astype(BF16).astype(F32)
        return ((a + b) * 0.5).astype(BF16).astype(F32)

    def inner(r):
        return lambda f, b: x[f, pl.ds(r + b, 2)].reshape(256, 128)

    loads[0].wait()
    loads[1].wait()

    def own_part(i, carry):
        r = 2 * i + 1
        head, second = late(inner(r))
        z[0, pl.ds(r, 2)] = head.reshape(2, 128, 128)
        z[1, pl.ds(r, 2)] = second.reshape(2, 128, 128)
        return carry

    lax.fori_loop(0, 3, own_part, 0)
    pl.semaphore_wait(barrier, total)

    @pl.when(has_prev)
    def _():
        pl.semaphore_signal(near, inc=1, device_id=(tm - 1, row), device_id_type=MESH)

    @pl.when(first & has_prev2)
    def _():
        pl.semaphore_signal(near, inc=1, device_id=(tm - 2, row), device_id_type=MESH)

    far = first & has_prev
    lead = second & has_next
    send(up, "OU", own(1), own(9), above)
    send(down, "OD", own(8), own(0), below)
    hold = second & ((tm // 2) % 2 == 1)
    arrived(hold & cross_down, "OU", own(9))
    arrived(hold & cross_up, "OD", own(0))
    send(has_next, "E1", own(8), old(8), nxt)
    send(has_next, "E0", own(1), old(1), nxt)
    send(has_next, "S0", own(2), old(2), nxt)
    send(has_next, "M0", own(3, 2), old(3, 2), nxt)
    arrived(second & ~hold & cross_down, "OU", own(9))
    arrived(second & ~hold & cross_up, "OD", own(0))
    send(lead & cross_down, "HU", own(9), old(9), nxt, "FU")
    send(lead & cross_up, "HD", own(0), old(0), nxt, "FD")
    send(has_next, "M1", own(5, 3), old(5, 3), nxt)

    arrived(down & ~(second & cross_down), "OU", own(9))
    send(first & down, "HU", own(9), old(9), nxt, "FU")
    arrived(up & ~(second & cross_up), "OD", own(0))
    send(first & up, "HD", own(0), old(0), nxt, "FD")
    arrived(has_prev, "E1", old(8))
    send(far & down & ~cross_down, "FD", old(8), old(0), below)
    arrived(has_prev, "E0", old(1))
    send(far & up & ~cross_up, "FU", old(1), old(9), above)

    head_a, second_a = late(lambda f, b: jnp.concatenate([x[f, b], x[f, 7 + b]], axis=0))
    z[0, 7] = head_a[128:]
    z[1, 7] = second_a[128:]
    arrived(up & has_prev, "FD", old(0))
    arrived(has_prev, "S0", old(2))
    head_b, second_b = early(lambda f, b: x[f, b])
    top = pooled(head_a[:128] + head_b, second_a[:128] + second_b)
    pool[0, pl.ds(0, 128)] = top
    rim[0] = top.astype(BF16)
    send(up, "PR", rim.at[0], rim.at[1], above)

    def rest_part(i, carry):
        r = 2 * i + 1
        head, second = early(inner(r))
        head = head + z[0, pl.ds(r, 2)].reshape(256, 128)
        second = second + z[1, pl.ds(r, 2)].reshape(256, 128)
        pool[pl.ds(r, 2), pl.ds(0, 128)] = pooled(head, second).reshape(2, 128, 128)
        return carry

    def reduce(p):
        strip = [
            pool[2 * p + b, pl.ds(e, 64, stride=2), :].astype(BF16)
            for b in range(3)
            for e in range(3)
        ]
        red[2, p + 1] = dot(jnp.concatenate(strip, axis=1), wd[...].reshape(1152, 256)).astype(BF16)

    hop2 = first & has_next2

    def pass_on(p):
        send(has_next, "N%d" % p, part(2, p + 1), part(1, p + 1), nxt)
        send(hop2, "Q%d" % p, part(2, p + 1), part(0, p + 1), nx2)

    def rim_up():
        send(up, "T2U", part(2, 1), part(2, 5), above)
        send(up & has_next, "T1U", part(2, 1), part(1, 5), (tm + 1, row - 1))
        send(up & hop2, "T0U", part(2, 1), part(0, 5), (tm + 2, row - 1))

    def rim_down():
        send(down, "T2D", part(2, 4), part(2, 0), below)
        send(down & has_next, "T1D", part(2, 4), part(1, 0), (tm + 1, row + 1))
        send(down & hop2, "T0D", part(2, 4), part(0, 0), (tm + 2, row + 1))

    loads[2].wait()

    @pl.when(has_next)
    def _():
        pl.semaphore_wait(near, 1 + hop2.astype(jnp.int32))

    arrived(has_prev, "M0", old(3, 2))
    rest_part(0, 0)
    reduce(0)
    rim_up()
    pass_on(0)
    arrived(has_prev, "M1", old(5, 3))
    rest_part(1, 0)
    reduce(1)
    pass_on(1)
    rest_part(2, 0)
    reduce(2)
    pass_on(2)
    arrived(down & has_prev, "FU", old(9))
    head_b, second_b = early(lambda f, b: x[f, 7 + b])
    pool[7, pl.ds(0, 128)] = pooled(z[0, 7] + head_b, z[1, 7] + second_b)
    arrived(down, "PR", rim.at[1])
    pool[8, pl.ds(0, 128)] = rim[1].astype(F32)
    reduce(3)
    rim_down()
    pass_on(3)

    def tile(a, b, e):
        return wc[a, b, pl.ds(e * 256, 256), :]

    def coarse(a, e):
        none = jnp.zeros((64, 256), BF16)
        r1, r2, r3, r5 = (red[a, r] for r in (1, 2, 3, 5))
        stacks = ((none, r1, r2, r3), (r1, r2, r3, none), (r2, r3, none, r5))
        left = jnp.concatenate([jnp.concatenate(rows, axis=0) for rows in stacks], axis=1)
        return dot(left, jnp.concatenate([tile(a, b, e) for b in range(3)], axis=0))

    def last(r, b, e):
        left = jnp.concatenate([red[a, r] for a in range(3)], axis=1)
        return dot(left, jnp.concatenate([tile(a, b, e) for a in range(3)], axis=0))

    loads[3].wait()
    for p in range(3):
        arrived(has_prev, "N%d" % p, part(1, p + 1))
        send(far, "G%d" % p, part(1, p + 1), part(0, p + 1), nxt, "Q%d" % p)
    arrived(down & has_prev, "T1U", part(1, 5))
    send(far & down, "K0U", part(1, 5), part(0, 5), nxt, "T0U")
    arrived(down, "T2U", part(2, 5))
    for e in range(3):
        y[e] = coarse(2, e) + coarse(1, e)
    for p in range(3):
        arrived(has_prev2, "Q%d" % p, part(0, p + 1))
    arrived(down & has_prev2, "T0U", part(0, 5))
    for e in range(3):
        y[e] = y[e] + coarse(0, e)
    arrived(has_prev, "N3", part(1, 4))
    send(far, "G3", part(1, 4), part(0, 4), nxt, "Q3")
    arrived(up & has_prev, "T1D", part(1, 0))
    send(far & up, "K0D", part(1, 0), part(0, 0), nxt, "T0D")
    arrived(up, "T2D", part(2, 0))
    arrived(has_prev2, "Q3", part(0, 4))
    arrived(up & has_prev2, "T0D", part(0, 0))
    parts = [
        jnp.concatenate(
            [
                y[e, pl.ds(0, 64)] + last(0, 0, e),
                y[e, pl.ds(64, 64)],
                y[e, pl.ds(128, 64)] + last(4, 2, e),
                y[e, pl.ds(192, 64)] + last(4, 1, e),
            ],
            axis=0,
        )
        for e in range(3)
    ]
    out[...] = silu(spread(*parts, 64)).astype(BF16).reshape(1, 4, 64, 256)

    for ok, copy in sent:

        @pl.when(ok)
        def _():
            copy.wait_send()


def solution(mesh):
    import functools

    tms, rws = mesh.shape["tm"], mesh.shape["rows"]
    anywhere = pl.BlockSpec(memory_space=pl.ANY)

    def local(frames, conv_fine, conv_down, conv_coarse):
        return pl.pallas_call(
            functools.partial(kernel, tms, rws),
            out_shape=jax.ShapeDtypeStruct((1, 4, 64, 256), BF16),
            in_specs=[anywhere] * 4,
            out_specs=pl.BlockSpec(memory_space=pltpu.VMEM),
            scratch_shapes=[
                pltpu.VMEM((4, 10, 128, 128), BF16),
                pltpu.VMEM((3, 3, 384, 128), BF16),
                pltpu.VMEM((3, 384, 256), BF16),
                pltpu.VMEM((3, 3, 768, 256), BF16),
                pltpu.VMEM((2, 8, 128, 128), F32),
                pltpu.VMEM((9, 136, 128), F32),
                pltpu.VMEM((2, 128, 128), BF16),
                pltpu.VMEM((3, 6, 64, 256), BF16),
                pltpu.VMEM((3, 256, 256), F32),
                pltpu.SemaphoreType.DMA((len(IDS),)),
                pltpu.SemaphoreType.DMA((len(IDS),)),
                pltpu.SemaphoreType.DMA((4,)),
                pltpu.SemaphoreType.REGULAR,
            ],
            compiler_params=pltpu.CompilerParams(
                collective_id=0, has_side_effects=True, vmem_limit_bytes=54800 * 1024
            ),
            name="encoder",
        )(frames, conv_fine, conv_down, conv_coarse)

    placed = (P("tm", "rows", None, None), P(), P(), P())
    return jax.shard_map(
        local, mesh=mesh, in_specs=placed, out_specs=P("tm", "rows", None, None), check_vma=False
    )
```
